32 devices in a mesh: front: 4 (over x, core), grid: 8 (over z, y).
Axes of the slice: x: 2, y: 2, z: 4, core: 2. Of those that a mesh axis runs over, the one named last changes fastest.
Arguments:
- index_map: int32 [4, 8192], P('front'), may hold values from 0 to 16383, as said below
- lengths: int32 [4], P('front'), may hold values from 1 to 8192, 24576 in all
- update_front: float32 [4, 8192, 8192], P('front', 'grid'), may hold values from -0.0625 to 0.0625
- front_matrix: float32 [16384, 16384], P(('front', 'grid')), may hold values from -0.046875 to 0.046875
- random: float32 [16384, 256], P(('front', 'grid')), may hold values from -6 to 6
Outputs:
- parent_sample: float32 [16384, 256], P(('front', 'grid'))
The draws below stay inside these ranges and needn't reach their ends.
Inputs may be any that keep to these rules, and one draw needn't show every extreme that they name: `index_map`: within one child the 8192 entries are distinct parent rows. `lengths`: rows of a child at or past its length are not live; the largest length equals 8192.
All inputs are finite; a program needn't handle non-finite values. No bound on the sum of `lengths` on one device may be relied on, other than what follows from the above.
Results may differ from the reference program's by a relative error of at most 0.0003.
Values sent between devices are 32-bit elements; how exact they have to be, the bound alone decides.
A program may use at most 192 MiB of HBM per device.

```python
import math
import jax
import jax.numpy as jnp
import numpy as np
from jax import lax

WP = 16384
UC = 8192
K = 256
CHILDREN = 4


def draw_index_map(key, part):
    child_keys = jax.random.split(jax.random.fold_in(key, 17), CHILDREN)
    picked = jax.vmap(lambda child_key: jax.random.permutation(child_key, WP)[:UC])(child_keys)
    return picked.astype(jnp.int32)


def levels(stream_key, shape, shards, smallest, largest):
    factor_of, own = 1.0, jax.random.fold_in(stream_key, 6)
    for position, shards_of in shards:
        heights = jnp.exp(jax.random.uniform(jax.random.fold_in(own, position), (shards_of,), jnp.float32, smallest / len(shards), largest / len(shards)))
        factor_of = factor_of * jnp.repeat(heights, shape[position] // shards_of).reshape([-1 if axis == position else 1 for axis in range(len(shape))])
    return factor_of


def length_profile(count, total, bound, skew):
    portions = [(1 << 20) // math.isqrt(standing ** skew) + 1 for standing in range(2, count + 1)]
    rest, holding = total - bound - (count - 1), [1] * (count - 1)
    while rest > 0:
        candidates = [i for i in range(count - 1) if holding[i] < bound]
        mass, remaining = sum([portions[i] for i in candidates]), rest
        for i in candidates:
            addition = min(bound - holding[i], max(1, remaining * portions[i] // mass), rest)
            holding[i] = holding[i] + addition
            rest = rest - addition
    return np.array([bound] + holding)


def ragged_sizes(stream_key, amount, total, reach, skew):
    if amount == 2:
        one = jax.random.randint(stream_key, (), max(1, total - reach), min(reach, total - 1) + 1)
        return jnp.stack([one, total - one])
    sizes = jnp.asarray(length_profile(amount, total, reach, skew), jnp.int32)
    twos = (amount - 1) // 2
    source_of, receiver = sizes[1:1 + 2 * twos:2], sizes[2:2 + 2 * twos:2]
    room = jnp.minimum(source_of - 1, reach - receiver)
    shifted = jax.random.randint(jax.random.fold_in(stream_key, 1), (twos,), 0, 1 << 20) % (room + 1)
    sizes = sizes.at[1:1 + 2 * twos:2].set(source_of - shifted).at[2:2 + 2 * twos:2].set(receiver + shifted)
    return sizes[jax.random.permutation(jax.random.fold_in(stream_key, 2), amount)]


def gaussian(key, dims, width, most, pieces=(), held_as=jnp.bfloat16):
    loudness = levels(key, dims, pieces, -0.22, 0.18) if pieces else 1.0
    drawn = jax.random.normal(key, dims, jnp.float32) * width * loudness
    return jnp.minimum(jnp.maximum(drawn, -most), most).astype(held_as)


def setup_inputs(seed: int = 0) -> dict:
    splits = jax.random.split(jax.random.key(seed), 6)
    return {
        "index_map": draw_index_map(jax.random.fold_in(splits[5], 71), 0),
        "lengths": ragged_sizes(splits[1], CHILDREN, 3 * UC, UC, 2).astype(jnp.int32),
        "update_front": gaussian(splits[2], (CHILDREN, UC, UC), UC ** -0.5, 0.0625, ((0, 4), (1, 8)), jnp.float32),
        "front_matrix": gaussian(splits[3], (WP, WP), WP ** -0.5, 0.046875, ((0, 32),), jnp.float32),
        "random": gaussian(splits[4], (WP, K), 1.0, 6.0, ((0, 32),), jnp.float32),
    }


def reference(index_map, lengths, update_front, front_matrix, random):
    parent_sample = jnp.dot(front_matrix, random, preferred_element_type=jnp.float32, precision=lax.Precision.HIGHEST)
    row_numbers = jnp.arange(UC, dtype=jnp.int32)

    def one_child(packed):
        child_rows, child_length, child_block = packed
        child_random = jnp.take(random, child_rows, axis=0)
        child_sample = jnp.dot(child_block, child_random, preferred_element_type=jnp.float32, precision=lax.Precision.HIGHEST)
        return jnp.where((row_numbers < child_length)[:, None], child_sample, jnp.float32(0.0))

    samples = lax.map(one_child, (index_map, lengths, update_front))
    for child in range(CHILDREN):
        parent_sample = parent_sample.at[index_map[child]].add(samples[child])
    return parent_sample
```

```python
import jax
import jax.numpy as jnp
from jax import lax
from jax.sharding import PartitionSpec as P


def product(a, b):
    return jnp.dot(a, b, preferred_element_type=jnp.float32, precision=lax.Precision.HIGH)


def shards(index_map, lengths, update_front, front_matrix, random):
    gathered_random = lax.all_gather(random, ("front", "grid"), axis=0, tiled=True)
    own_rows = front_matrix.shape[0]
    half = own_rows // 2
    index_rows = index_map[0]
    child_random = jnp.take(gathered_random, index_rows, axis=0)
    child_sample = product(update_front[0], child_random)
    local_rows = child_sample.shape[0]
    first_row = lax.axis_index("grid") * local_rows
    row_numbers = first_row + jnp.arange(local_rows, dtype=jnp.int32)
    live_rows = row_numbers < lengths[0]
    child_sample = jnp.where(live_rows[:, None], child_sample, jnp.float32(0.0))
    child_sample, gathered_random = lax.optimization_barrier((child_sample, gathered_random))
    group_sample = lax.all_gather(child_sample, "grid", axis=0, tiled=True)
    upper = product(front_matrix[:half], gathered_random)
    group_sample, upper = lax.optimization_barrier((group_sample, upper))
    group_count = lax.axis_size("front")
    grid_count = lax.axis_size("grid")
    grid_place = lax.axis_index("grid")
    block_ids = jnp.arange(group_count, dtype=jnp.int32)[:, None] * grid_count + grid_place
    targets = (block_ids * own_rows + jnp.arange(own_rows, dtype=jnp.int32)[None, :]).reshape(-1)
    one_hot = (targets[:, None] == index_rows[None, :]).astype(jnp.bfloat16)
    coarse = lax.reduce_precision(group_sample, 8, 7)
    rest = group_sample - coarse
    halves = jnp.concatenate([coarse, rest], axis=1).astype(jnp.bfloat16)
    both = jnp.dot(one_hot, halves, preferred_element_type=jnp.float32)
    width = group_sample.shape[1]
    terms = both[:, :width] + both[:, width:]
    terms = terms.reshape(group_count, own_rows, width)
    terms, gathered_random = lax.optimization_barrier((terms, gathered_random))
    added = lax.psum_scatter(terms, "front", scatter_dimension=0, tiled=True)[0]
    lower = product(front_matrix[half:], gathered_random)
    added, lower = lax.optimization_barrier((added, lower))
    return jnp.concatenate([upper, lower], axis=0) + added


def solution(mesh):
    placed = (
        P("front", None),
        P("front"),
        P("front", "grid", None),
        P(("front", "grid"), None),
        P(("front", "grid"), None),
    )
    return jax.shard_map(
        shards, mesh=mesh, in_specs=placed, out_specs=P(("front", "grid"), None), check_vma=False
    )
```
